32 devices in a mesh: ang: 8 (over z, x), tile: 4 (over y, core).
Axes of the slice: x: 2, y: 2, z: 4, core: 2. Of those that a mesh axis runs over, the one named last changes fastest.
Arguments:
- sinogram: float32 [2, 64, 2048], P(None, 'ang'), may hold values from -6 to 6
- ray_offsets: int32 [64, 256], P('ang'), may hold values from 0 to 2047
- merge_matrices: float32 [3, 2, 2, 256, 256], replicated, may hold values from -1 to 1.5, as said below
Outputs:
- reconstruction: float32 [2, 2048, 2048], P(None, 'ang')
The draws below stay inside these ranges and needn't reach their ends.
Inputs may be any that keep to these rules, and one draw needn't show every extreme that they name: merge_matrices[l, b, k] is zero outside the columns b * (96) to b * 96 + 256 / 2 + 31.
All inputs are finite; a program needn't handle non-finite values.
Results may differ from the reference program's by a relative error of at most 0.0003.
Values sent between devices are 32-bit elements; how exact they have to be, the bound alone decides.
A program may use at most 768 MiB of HBM per device.

```python
import math
import jax
import jax.numpy as jnp
from jax import lax

NPIX = 2048
ANG_DEV = 8
SLICES = 2
ANGLES = 64
R = 256
HALO = 32
LEVELS = 3
N_ANG = 8


def draw_merge_matrices(key, part):
    shape = (LEVELS, 2, 2, R, R)
    noise = jnp.clip(jax.random.normal(key, shape, jnp.float32), -4.0, 4.0)
    width = R // 2 + HALO
    fine = jnp.arange(R, dtype=jnp.float32)[None, :, None]
    coarse = jnp.arange(R, dtype=jnp.float32)[None, None, :]
    half_bit = jnp.arange(2, dtype=jnp.float32)[:, None, None]
    centre = half_bit * (R // 2) + 0.5 * fine
    kernel = jnp.maximum(0.0, 1.0 - jnp.abs(coarse - centre))
    low_col = half_bit * (R // 2 - HALO)
    inside = jnp.logical_and(coarse >= low_col, coarse < low_col + width).astype(jnp.float32)
    kernel = kernel[None, :, None, :, :]
    inside = inside[None, :, None, :, :]
    return inside * (0.5 * kernel + 0.5 * noise / math.sqrt(width))


def set_ends(values, stream_key, smallest, largest):
    longest = values.shape.index(max(values.shape))
    spots = []
    for shift in (0, 1):
        where = [jax.random.randint(jax.random.fold_in(stream_key, axis), (), 0, length) for axis, length in enumerate(values.shape)]
        where[longest] = (where[longest] + shift) % values.shape[longest]
        spots.append(tuple(where))
    return values.at[spots[0]].set(smallest).at[spots[1]].set(largest)


def level_of(own_key, dims, cuts, smallest, largest):
    def one(position, parts):
        draws = jax.random.uniform(jax.random.fold_in(jax.random.fold_in(own_key, 6), position), (parts,), jnp.float32, smallest / len(cuts), largest / len(cuts))
        return jnp.repeat(jnp.exp(draws), dims[position] // parts).reshape((-1,) + (1,) * (len(dims) - position - 1))

    gain = one(*cuts[0])
    for cut in cuts[1:]:
        gain = gain * one(*cut)
    return gain


def scatter_about(key, dims, scale, bound, pieces=(), kind=jnp.bfloat16):
    entries = jax.random.normal(key, dims, jnp.float32) * scale
    if len(pieces) > 0:
        entries = level_of(key, dims, pieces, -0.22, 0.18) * entries
    return jnp.clip(entries, min=-bound, max=bound).astype(kind)


def setup_inputs(seed: int = 0) -> dict:
    splits = jax.random.split(jax.random.key(seed), 4)
    sinogram = scatter_about(splits[0], (SLICES, ANGLES, NPIX), 1.0, 6.0, ((1, 8),), jnp.float32)
    ray_offsets = set_ends(jax.random.randint(splits[1], (ANGLES, R), 0, NPIX), jax.random.fold_in(splits[1], 1), 0, NPIX - 1).astype(jnp.int32)
    merge_matrices = draw_merge_matrices(jax.random.fold_in(splits[3], 71), 0)
    return dict(sinogram=sinogram, ray_offsets=ray_offsets, merge_matrices=merge_matrices)


def apply_rows(matrix, field):
    return jnp.einsum('rk,...kw->...rw', matrix, field, precision=lax.Precision.HIGHEST)

def smear_rows(sinogram, offsets, columns):
    slices = sinogram.shape[0]
    angles = sinogram.shape[1]
    bin_count = sinogram.shape[2]
    row_count = offsets.shape[1]
    blocks = angles // 8
    grouped = sinogram.reshape(slices, blocks, 8, bin_count).transpose(1, 0, 2, 3)
    grouped_offsets = offsets.reshape(blocks, 8, row_count)
    angle_ids = jnp.arange(8, dtype=jnp.int32)[:, None, None]

    def add_block(running, inputs):
        rows_block, offset_block = inputs
        bin_index = jnp.remainder(columns[None, None, :] + offset_block[:, :, None], bin_count).astype(jnp.int32)
        samples = rows_block[:, angle_ids, bin_index]
        return (running + lax.optimization_barrier(jnp.sum(samples, axis=1)), None)
    zeros_init = jnp.zeros((slices, row_count, columns.shape[0]), jnp.float32)
    running, _ = lax.scan(add_block, zeros_init, (grouped, grouped_offsets))
    return running / math.sqrt(angles)

def reference(sinogram, ray_offsets, merge_matrices):
    grouped = sinogram.reshape(SLICES, N_ANG, ANG_DEV, NPIX).transpose(1, 0, 2, 3)
    offsets_grouped = ray_offsets.reshape(N_ANG, ANG_DEV, R)
    columns = jnp.arange(NPIX, dtype=jnp.int32)
    partial_value = lax.map(lambda inputs: smear_rows(inputs[0], inputs[1], columns), (grouped, offsets_grouped))
    for level_num in range(LEVELS):
        half_span = 2 ** (LEVELS - 1 - level_num)
        shaped = partial_value.reshape(N_ANG // (2 * half_span), 2, half_span, SLICES, R, NPIX)
        lower = shaped[:, 0]
        upper = shaped[:, 1]
        mats = merge_matrices[level_num]
        new_lower = apply_rows(mats[0, 0], lower) + apply_rows(mats[0, 1], upper)
        new_upper = apply_rows(mats[1, 0], upper) + apply_rows(mats[1, 1], lower)
        partial_value = jnp.stack([new_lower, new_upper], axis=1).reshape(N_ANG, SLICES, R, NPIX)
    return partial_value.transpose(1, 0, 2, 3).reshape(SLICES, NPIX, NPIX)
```

```python
import functools
import math

import jax
import jax.numpy as jnp
from jax import lax
from jax.experimental import pallas as pl
from jax.experimental.pallas import tpu as pltpu
from jax.sharding import PartitionSpec as P

LANES = 128
SUBLANES = 8
UNROLL = 4


def split_bf16(value):
    high = value.astype(jnp.bfloat16)
    return high, (value - high.astype(jnp.float32)).astype(jnp.bfloat16)


def merge_kernel(dims, starts_ref, groups_ref, row0_ref, tiles_ref, weights_ref, out_ref, wide_ref, samples_ref):
    slices, bins, angles, rows, width, groups = dims
    per_tile = SUBLANES // slices
    count = bins // LANES // per_tile
    spread = wide_ref.shape[0] // (groups * angles)

    def widen(angle, carry):
        for i in range(count):
            tile = tiles_ref[angle * count + i]
            for u in range(spread // count):
                turn = (-slices * u) % SUBLANES
                turned = pltpu.roll(tile, turn, 0) if turn else tile
                wide_ref[angle * spread + u * count + i] = turned
        return carry

    lax.fori_loop(0, groups * angles, widen, 0)
    lane = lax.broadcasted_iota(jnp.int32, (SUBLANES, LANES), 1)
    row0 = row0_ref[0]

    def by_group(index, carry):
        group = groups_ref[index]

        def by_rows(step, inner):
            for u in range(UNROLL):
                q = step * UNROLL + u
                sums = [None] * count
                for a in range(angles):
                    angle = group * angles + a
                    start = starts_ref[angle * rows + row0 + q]
                    base = angle * spread + lax.shift_right_logical(start, 7)
                    fine = jnp.bitwise_and(start, LANES - 1)
                    turn = jnp.bitwise_and(LANES - fine, LANES - 1)
                    mask = lane >= fine
                    held = [wide_ref[base + i] for i in range(count + 1)]
                    for i in range(count):
                        moved = pltpu.roll(jnp.where(mask, held[i], held[i + 1]), turn, 1)
                        sums[i] = moved if a == 0 else sums[i] + moved
                for i in range(count):
                    at = ((index * width + q) * count + i) * SUBLANES
                    samples_ref[pl.ds(pl.multiple_of(at, SUBLANES), SUBLANES), :] = sums[i]
            return inner

        return lax.fori_loop(0, width // UNROLL, by_rows, carry)

    lax.fori_loop(0, groups, by_group, 0)
    high, low = split_bf16(weights_ref[...])
    depth = groups * width
    pairs = bins // (2 * LANES)

    def by_columns(n, carry):
        s = n // pairs
        c0 = (n % pairs) * 2
        first = (c0 % count) * SUBLANES + (c0 // count) * slices + s
        parts = [samples_ref[pl.ds(first + k * SUBLANES, depth, stride=count * SUBLANES), :] for k in range(2)]
        field_high, field_low = split_bf16(jnp.concatenate(parts, axis=1))
        dot = functools.partial(jnp.dot, preferred_element_type=jnp.float32)
        total = dot(high, field_high) + (dot(high, field_low) + dot(low, field_high))
        out_ref[s, :, pl.ds(pl.multiple_of(c0 * LANES, 2 * LANES), 2 * LANES)] = total
        return carry

    lax.fori_loop(0, slices * pairs, by_columns, 0)


def body(sinogram, ray_offsets, merge_matrices):
    slices, angles, bins = sinogram.shape
    rows = ray_offsets.shape[1]
    margin = rows // 8
    width = rows // 2 + margin
    groups = lax.axis_size("ang")
    levels = groups.bit_length() - 1
    own = lax.axis_index("ang")
    per_tile = SUBLANES // slices
    count = bins // LANES // per_tile
    spread = count * (per_tile + 1)

    own_tiles = sinogram.reshape(slices, angles, per_tile, count, LANES).transpose(1, 3, 2, 0, 4)
    own_tiles = own_tiles.reshape(angles * count, SUBLANES, LANES)
    tiles = lax.all_gather(own_tiles, "ang", axis=0, tiled=True)
    starts = lax.all_gather(ray_offsets.reshape(-1), "ang", axis=0, tiled=True)

    bits = [jnp.right_shift(own, levels - 1 - level) & 1 for level in range(levels)]
    weights = None
    for level in range(levels - 1, -1, -1):
        matrices = lax.dynamic_index_in_dim(merge_matrices[level], bits[level], 0, keepdims=False)
        if level == 0:
            matrices = lax.dynamic_slice_in_dim(matrices, bits[0] * (rows // 2 - margin), width, 2)
        if weights is None:
            weights = matrices.transpose(1, 0, 2)
        else:
            weights = jnp.einsum("rxk,mkj->rxmj", weights, matrices, precision=lax.Precision.HIGHEST)
        weights = weights.reshape(rows, -1, matrices.shape[2])
    weights = weights.reshape(rows, groups * width) / math.sqrt(angles)

    flips = [int(format(i, f"0{levels}b")[::-1], 2) for i in range(groups)]
    group_order = jnp.bitwise_xor(own, jnp.array(flips, jnp.int32)).astype(jnp.int32)
    row0 = (bits[0] * (rows // 2 - margin)).astype(jnp.int32).reshape(1)

    smem = pl.BlockSpec(memory_space=pltpu.SMEM)
    vmem = pl.BlockSpec(memory_space=pltpu.VMEM)
    return pl.pallas_call(
        functools.partial(merge_kernel, (slices, bins, angles, rows, width, groups)),
        out_shape=jax.ShapeDtypeStruct((slices, rows, bins), jnp.float32),
        in_specs=[smem, smem, smem, vmem, vmem],
        out_specs=vmem,
        scratch_shapes=[
            pltpu.VMEM((groups * angles * spread, SUBLANES, LANES), jnp.float32),
            pltpu.VMEM((groups * width * count * SUBLANES, LANES), jnp.float32),
        ],
        compiler_params=pltpu.CompilerParams(vmem_limit_bytes=60 * 1024 * 1024),
    )(starts, group_order, row0, tiles, weights)


def solution(mesh):
    placed = (P(None, "ang", None), P("ang", None), P())
    return jax.shard_map(
        body, mesh=mesh, in_specs=placed, out_specs=P(None, "ang", None), check_vma=False
    )
```

```python
import functools
import math

import jax
import jax.numpy as jnp
from jax import lax
from jax.experimental import pallas as pl
from jax.experimental.pallas import tpu as pltpu
from jax.sharding import PartitionSpec as P

LANES = 128
SUBLANES = 8
UNROLL = 20


def gather_kernel(groups, tiles_ref, starts_ref, all_tiles_ref, all_starts_ref, send_sems, recv_sems, own_sems):
    own = lax.axis_index("ang")
    barrier = pltpu.get_barrier_semaphore()
    for k in range(1, groups):
        pl.semaphore_signal(barrier, inc=1, device_id={"ang": own ^ k}, device_id_type=pl.DeviceIdType.MESH)
    pl.semaphore_wait(barrier, groups - 1)
    pairs = ((starts_ref, all_starts_ref), (tiles_ref, all_tiles_ref))
    copies = []
    for k in range(1, groups):
        for n, (source, target) in enumerate(pairs):
            copies.append(
                pltpu.make_async_remote_copy(
                    src_ref=source,
                    dst_ref=target.at[own],
                    send_sem=send_sems.at[n, k],
                    recv_sem=recv_sems.at[n, k],
                    device_id={"ang": own ^ k},
                    device_id_type=pl.DeviceIdType.MESH,
                )
            )
    for n, (source, target) in enumerate(pairs):
        copies.append(pltpu.make_async_copy(source, target.at[own], own_sems.at[n]))
    for copy in copies:
        copy.start()
    for copy in copies:
        copy.wait()


def gather_groups(tiles, starts, groups):
    vmem = pl.BlockSpec(memory_space=pltpu.VMEM)
    sems = pltpu.SemaphoreType.DMA((2, groups))
    return pl.pallas_call(
        functools.partial(gather_kernel, groups),
        out_shape=[jax.ShapeDtypeStruct((groups,) + x.shape, x.dtype) for x in (tiles, starts)],
        in_specs=[vmem, vmem],
        out_specs=[vmem, vmem],
        scratch_shapes=[sems, sems, pltpu.SemaphoreType.DMA((2,))],
        compiler_params=pltpu.CompilerParams(collective_id=0, has_side_effects=True),
    )(tiles, starts)


def split_bf16(value):
    high = value.astype(jnp.bfloat16)
    return high, (value - high.astype(jnp.float32)).astype(jnp.bfloat16)


def merge_kernel(dims, starts_ref, groups_ref, row0_ref, tiles_ref, weights_ref, out_ref, wide_ref, samples_ref, high_ref, low_ref):
    slices, bins, angles, rows, width, groups = dims
    per_tile = SUBLANES // slices
    count = bins // LANES // per_tile
    spread = count * (per_tile + 1)

    def widen(angle, carry):
        for i in range(count):
            tile = tiles_ref[angle * count + i]
            for u in range(spread // count):
                turn = (-slices * u) % SUBLANES
                turned = pltpu.roll(tile, turn, 0) if turn else tile
                at = (angle * spread + u * count + i) * SUBLANES
                wide_ref[pl.ds(pl.multiple_of(at, SUBLANES), SUBLANES), :] = turned
        return carry

    lax.fori_loop(0, groups * angles, widen, 0)
    reverse_lane = LANES - 1 - lax.broadcasted_iota(jnp.int32, (SUBLANES, LANES), 1)
    row0 = row0_ref[0]
    unroll = math.gcd(width, UNROLL)

    def by_group(index, carry):
        group = groups_ref[index]

        def by_rows(step, inner):
            first = (2 * rows * group + row0 + step * unroll) * angles
            for u in range(unroll):
                q = step * unroll + u
                sums = [None] * count
                for a in range(angles):
                    turn = starts_ref[first + u * angles + a + angles * rows]
                    base = starts_ref[first + u * angles + a]
                    mask = reverse_lane < turn
                    held = []
                    for i in range(count + 1):
                        at = pl.multiple_of(base + i * SUBLANES, SUBLANES)
                        held.append(wide_ref[pl.ds(at, SUBLANES), :])
                    for i in range(count):
                        moved = pltpu.roll(jnp.where(mask, held[i], held[i + 1]), turn, 1)
                        sums[i] = moved if a == 0 else sums[i] + moved
                for i in range(count):
                    at = ((index * width + q) * count + i) * SUBLANES
                    samples_ref[pl.ds(pl.multiple_of(at, SUBLANES), SUBLANES), :] = sums[i]
            return inner

        return lax.fori_loop(0, width // unroll, by_rows, carry)

    lax.fori_loop(0, groups, by_group, 0)
    high_ref[...], low_ref[...] = split_bf16(weights_ref[...])
    depth = groups * width
    pairs = bins // (2 * LANES)

    def by_columns(n, carry):
        s = n // pairs
        c0 = (n % pairs) * 2
        first = (c0 % count) * SUBLANES + (c0 // count) * slices + s
        parts = [samples_ref[pl.ds(first + k * SUBLANES, depth, stride=count * SUBLANES), :] for k in range(2)]
        field_high, field_low = split_bf16(jnp.concatenate(parts, axis=1))
        dot = functools.partial(jnp.dot, preferred_element_type=jnp.float32)
        total = dot(high_ref[...], field_high) + (dot(high_ref[...], field_low) + dot(low_ref[...], field_high))
        out_ref[s, :, pl.ds(pl.multiple_of(c0 * LANES, 2 * LANES), 2 * LANES)] = total
        return carry

    lax.fori_loop(0, slices * pairs, by_columns, 0)


def body(sinogram, ray_offsets, merge_matrices):
    slices, angles, bins = sinogram.shape
    assert slices == 2 and lax.axis_size("tile") % 2 == 0
    rows = ray_offsets.shape[1]
    margin = rows // 8
    width = rows // 2 + margin
    groups = lax.axis_size("ang")
    levels = groups.bit_length() - 1
    own = lax.axis_index("ang")
    core = lax.axis_index("tile") % slices
    per_tile = SUBLANES
    count = bins // LANES // per_tile
    spread = count * (per_tile + 1)

    own_tiles = lax.dynamic_index_in_dim(sinogram, core, 0, keepdims=False)
    own_tiles = own_tiles.reshape(angles, per_tile, count, LANES).transpose(0, 2, 1, 3)
    own_tiles = own_tiles.reshape(angles * count, SUBLANES, LANES)
    angle = own * angles + jnp.arange(angles, dtype=jnp.int32)[:, None]
    bases = (angle * spread + jnp.right_shift(ray_offsets, 7)) * SUBLANES
    turns = LANES - jnp.bitwise_and(ray_offsets, LANES - 1)
    own_starts = jnp.stack([bases, turns]).transpose(0, 2, 1).reshape(-1, LANES).astype(jnp.int32)
    tiles, starts = gather_groups(own_tiles, own_starts, groups)
    tiles = tiles.reshape(-1, SUBLANES, LANES)
    starts = starts.reshape(-1)

    bits = [jnp.right_shift(own, levels - 1 - level) & 1 for level in range(levels)]
    weights = None
    for level in range(levels - 1, -1, -1):
        matrices = lax.dynamic_index_in_dim(merge_matrices[level], bits[level], 0, keepdims=False)
        if level == 0:
            matrices = lax.dynamic_slice_in_dim(matrices, bits[0] * (rows // 2 - margin), width, 2)
        if weights is None:
            weights = matrices.transpose(1, 0, 2)
        else:
            weights = jnp.einsum("rxk,mkj->rxmj", weights, matrices, precision=lax.Precision.HIGHEST)
        weights = weights.reshape(rows, -1, matrices.shape[2])
    weights = weights.reshape(rows, groups * width) / math.sqrt(angles)

    flips = [int(format(i, f"0{levels}b")[::-1], 2) for i in range(groups)]
    group_order = jnp.bitwise_xor(own, jnp.array(flips, jnp.int32)).astype(jnp.int32)
    row0 = (bits[0] * (rows // 2 - margin)).astype(jnp.int32).reshape(1)

    smem = pl.BlockSpec(memory_space=pltpu.SMEM)
    vmem = pl.BlockSpec(memory_space=pltpu.VMEM)
    finished = pl.pallas_call(
        functools.partial(merge_kernel, (1, bins, angles, rows, width, groups)),
        out_shape=jax.ShapeDtypeStruct((1, rows, bins), jnp.float32),
        in_specs=[smem, smem, smem, vmem, vmem],
        out_specs=vmem,
        scratch_shapes=[
            pltpu.VMEM((groups * angles * spread * SUBLANES, LANES), jnp.float32),
            pltpu.VMEM((groups * width * count * SUBLANES, LANES), jnp.float32),
            pltpu.VMEM((rows, groups * width), jnp.bfloat16),
            pltpu.VMEM((rows, groups * width), jnp.bfloat16),
        ],
        compiler_params=pltpu.CompilerParams(vmem_limit_bytes=60 * 1024 * 1024),
    )(starts, group_order, row0, tiles, weights)
    swaps = [(i, i ^ 1) for i in range(lax.axis_size("tile"))]
    other = lax.ppermute(finished, "tile", swaps)
    first = jnp.where(core == 0, finished, other)
    second = jnp.where(core == 0, other, finished)
    return jnp.concatenate([first, second], axis=0)


def solution(mesh):
    placed = (P(None, "ang", None), P("ang", None), P())
    return jax.shard_map(
        body, mesh=mesh, in_specs=placed, out_specs=P(None, "ang", None), check_vma=False
    )
```

```python
import functools
import math

import jax
import jax.numpy as jnp
from jax import lax
from jax.experimental import pallas as pl
from jax.experimental.pallas import tpu as pltpu
from jax.sharding import PartitionSpec as P

LANES = 128
SUBLANES = 8
UNROLL = 40


def gather_kernel(groups, tiles_ref, starts_ref, all_tiles_ref, all_starts_ref, send_sems, recv_sems, own_sems):
    own = lax.axis_index("ang")
    barrier = pltpu.get_barrier_semaphore()
    for k in range(1, groups):
        pl.semaphore_signal(barrier, inc=1, device_id={"ang": own ^ k}, device_id_type=pl.DeviceIdType.MESH)
    pl.semaphore_wait(barrier, groups - 1)
    pairs = ((starts_ref, all_starts_ref), (tiles_ref, all_tiles_ref))
    copies = []
    for k in range(1, groups):
        for n, (source, target) in enumerate(pairs):
            copies.append(
                pltpu.make_async_remote_copy(
                    src_ref=source,
                    dst_ref=target.at[own],
                    send_sem=send_sems.at[n, k],
                    recv_sem=recv_sems.at[n, k],
                    device_id={"ang": own ^ k},
                    device_id_type=pl.DeviceIdType.MESH,
                )
            )
    for n, (source, target) in enumerate(pairs):
        copies.append(pltpu.make_async_copy(source, target.at[own], own_sems.at[n]))
    for copy in copies:
        copy.start()
    for copy in copies:
        copy.wait()


def gather_groups(tiles, starts, groups):
    vmem = pl.BlockSpec(memory_space=pltpu.VMEM)
    sems = pltpu.SemaphoreType.DMA((2, groups))
    return pl.pallas_call(
        functools.partial(gather_kernel, groups),
        out_shape=[jax.ShapeDtypeStruct((groups,) + x.shape, x.dtype) for x in (tiles, starts)],
        in_specs=[vmem, vmem],
        out_specs=[vmem, vmem],
        scratch_shapes=[sems, sems, pltpu.SemaphoreType.DMA((2,))],
        compiler_params=pltpu.CompilerParams(collective_id=0, has_side_effects=True),
    )(tiles, starts)


def split_bf16(value):
    high = value.astype(jnp.bfloat16)
    return high, (value - high.astype(jnp.float32)).astype(jnp.bfloat16)


def merge_kernel(dims, starts_ref, groups_ref, row0_ref, tiles_ref, weights_ref, out_ref, wide_ref, samples_ref, high_ref, low_ref):
    slices, bins, angles, rows, width, groups = dims
    per_tile = SUBLANES // slices
    count = bins // LANES // per_tile
    spread = count * (per_tile + 1)

    def widen(angle, carry):
        for i in range(count):
            tile = tiles_ref[angle * count + i]
            for u in range(spread // count):
                turn = (-slices * u) % SUBLANES
                turned = pltpu.roll(tile, turn, 0) if turn else tile
                at = (angle * spread + u * count + i) * SUBLANES
                wide_ref[pl.ds(pl.multiple_of(at, SUBLANES), SUBLANES), :] = turned
        return carry

    lax.fori_loop(0, groups * angles, widen, 0)
    reverse_lane = LANES - 1 - lax.broadcasted_iota(jnp.int32, (SUBLANES, LANES), 1)
    row0 = row0_ref[0]
    unroll = math.gcd(width, UNROLL)

    def by_group(index, carry):
        group = groups_ref[index]

        def by_rows(step, inner):
            first = (2 * rows * group + row0 + step * unroll) * angles
            for u in range(unroll):
                q = step * unroll + u
                sums = [None] * count
                for a in range(angles):
                    turn = starts_ref[first + u * angles + a + angles * rows]
                    base = starts_ref[first + u * angles + a]
                    mask = reverse_lane < turn
                    held = []
                    for i in range(count + 1):
                        at = pl.multiple_of(base + i * SUBLANES, SUBLANES)
                        held.append(wide_ref[pl.ds(at, SUBLANES), :])
                    for i in range(count):
                        moved = pltpu.roll(jnp.where(mask, held[i], held[i + 1]), turn, 1)
                        sums[i] = moved if a == 0 else sums[i] + moved
                for i in range(count):
                    at = ((index * width + q) * count + i) * SUBLANES
                    samples_ref[pl.ds(pl.multiple_of(at, SUBLANES), SUBLANES), :] = sums[i]
            return inner

        return lax.fori_loop(0, width // unroll, by_rows, carry)

    lax.fori_loop(0, groups, by_group, 0)
    high_ref[...], low_ref[...] = split_bf16(weights_ref[...])
    depth = groups * width
    pairs = bins // (2 * LANES)

    def by_columns(n, carry):
        s = n // pairs
        c0 = (n % pairs) * 2
        first = (c0 % count) * SUBLANES + (c0 // count) * slices + s
        parts = [samples_ref[pl.ds(first + k * SUBLANES, depth, stride=count * SUBLANES), :] for k in range(2)]
        field_high, field_low = split_bf16(jnp.concatenate(parts, axis=1))
        dot = functools.partial(jnp.dot, preferred_element_type=jnp.float32)
        total = dot(high_ref[...], field_high) + (dot(high_ref[...], field_low) + dot(low_ref[...], field_high))
        out_ref[s, :, pl.ds(pl.multiple_of(c0 * LANES, 2 * LANES), 2 * LANES)] = total
        return carry

    lax.fori_loop(0, slices * pairs, by_columns, 0)


def body(sinogram, ray_offsets, merge_matrices):
    slices, angles, bins = sinogram.shape
    assert slices == 2 and lax.axis_size("tile") % 2 == 0
    rows = ray_offsets.shape[1]
    margin = rows // 8
    width = rows // 2 + margin
    groups = lax.axis_size("ang")
    levels = groups.bit_length() - 1
    own = lax.axis_index("ang")
    core = lax.axis_index("tile") % slices
    per_tile = SUBLANES
    count = bins // LANES // per_tile
    spread = count * (per_tile + 1)

    own_tiles = lax.dynamic_index_in_dim(sinogram, core, 0, keepdims=False)
    own_tiles = own_tiles.reshape(angles, per_tile, count, LANES).transpose(0, 2, 1, 3)
    own_tiles = own_tiles.reshape(angles * count, SUBLANES, LANES)
    angle = own * angles + jnp.arange(angles, dtype=jnp.int32)[:, None]
    bases = (angle * spread + jnp.right_shift(ray_offsets, 7)) * SUBLANES
    turns = LANES - jnp.bitwise_and(ray_offsets, LANES - 1)
    own_starts = jnp.stack([bases, turns]).transpose(0, 2, 1).reshape(-1, LANES).astype(jnp.int32)
    tiles, starts = gather_groups(own_tiles, own_starts, groups)
    tiles = tiles.reshape(-1, SUBLANES, LANES)
    starts = starts.reshape(-1)

    bits = [jnp.right_shift(own, levels - 1 - level) & 1 for level in range(levels)]
    weights = None
    for level in range(levels - 1, -1, -1):
        matrices = lax.dynamic_index_in_dim(merge_matrices[level], bits[level], 0, keepdims=False)
        if level == 0:
            matrices = lax.dynamic_slice_in_dim(matrices, bits[0] * (rows // 2 - margin), width, 2)
        if weights is None:
            weights = matrices.transpose(1, 0, 2)
        else:
            weights = jnp.einsum("rxk,mkj->rxmj", weights, matrices, precision=lax.Precision.HIGHEST)
        weights = weights.reshape(rows, -1, matrices.shape[2])
    weights = weights.reshape(rows, groups * width) / math.sqrt(angles)

    flips = [int(format(i, f"0{levels}b")[::-1], 2) for i in range(groups)]
    group_order = jnp.bitwise_xor(own, jnp.array(flips, jnp.int32)).astype(jnp.int32)
    row0 = (bits[0] * (rows // 2 - margin)).astype(jnp.int32).reshape(1)

    smem = pl.BlockSpec(memory_space=pltpu.SMEM)
    vmem = pl.BlockSpec(memory_space=pltpu.VMEM)
    finished = pl.pallas_call(
        functools.partial(merge_kernel, (1, bins, angles, rows, width, groups)),
        out_shape=jax.ShapeDtypeStruct((1, rows, bins), jnp.float32),
        in_specs=[smem, smem, smem, vmem, vmem],
        out_specs=vmem,
        scratch_shapes=[
            pltpu.VMEM((groups * angles * spread * SUBLANES, LANES), jnp.float32),
            pltpu.VMEM((groups * width * count * SUBLANES, LANES), jnp.float32),
            pltpu.VMEM((rows, groups * width), jnp.bfloat16),
            pltpu.VMEM((rows, groups * width), jnp.bfloat16),
        ],
        compiler_params=pltpu.CompilerParams(vmem_limit_bytes=60 * 1024 * 1024),
    )(starts, group_order, row0, tiles, weights)
    swaps = [(i, i ^ 1) for i in range(lax.axis_size("tile"))]
    other = lax.ppermute(finished, "tile", swaps)
    place = lax.broadcasted_iota(jnp.int32, (slices, 1, 1), 0)
    return jnp.where(place == core, finished, other)


def solution(mesh):
    placed = (P(None, "ang", None), P("ang", None), P())
    return jax.shard_map(
        body, mesh=mesh, in_specs=placed, out_specs=P(None, "ang", None), check_vma=False
    )
```
